256 devices in a mesh: groups: 2 (over y), mp: 16 (over z), expert: 4 (over x), dp: 2 (over core).
Axes of the slice: x: 4, y: 2, z: 16, core: 2. Of those that a mesh axis runs over, the one named last changes fastest.
The devices are a block of a 4x16x16 slice.
Arguments:
- hidden_in: bfloat16 [1024, 4096], P(('groups', 'expert', 'dp'), 'mp'), parts along dimension 0, may hold values from -6 to 6
- norm_gain: bfloat16 [2, 4096], P(None, 'mp'), may hold values from 0.25 to 1.75
- expert_ids: int32 [2, 1024, 2], P(None, ('groups', 'expert', 'dp')), parts along dimension 1, may hold values from 0 to 3, all different within a row; in each aligned block of 64 rows (0 to 63, 64 to 127, ..., all dimensions but the last counted through in order) at most 64 rows name the same one
- gate_counts: int32 [2, 1024, 2], P(None, ('groups', 'expert', 'dp')), parts along dimension 1, may hold values from 8 to 15
- exit_layer: int32 [1024], P(('groups', 'expert', 'dp')), parts along dimension 0, may hold values from 1 to 2
- w_gate: bfloat16 [2, 4, 7168, 4096], P(None, 'expert', ('mp', 'dp')), may hold values from -0.09375 to 0.09375
- w_up: bfloat16 [2, 4, 7168, 4096], P(None, 'expert', ('mp', 'dp')), may hold values from -0.09375 to 0.09375
- w_down: bfloat16 [2, 4, 7168, 4096], P(None, 'expert', ('mp', 'dp')), may hold values from -0.0625 to 0.0625
Outputs:
- hidden_out: bfloat16 [1024, 4096], P(('groups', 'expert', 'dp'), 'mp'), parts along dimension 0
The draws below stay inside these ranges and needn't reach their ends.
There are 2 independent parts, one for each index of `groups`. The reference program is written for one: setup_inputs(seed, part) draws one part's arguments, and reference() takes and returns one part's arrays. A program takes and returns all parts, laid end to end along the dimension named above; an argument that names none is the same for every part. Nothing has to cross between parts.
Inputs may be any that keep to these rules, and one draw needn't show every extreme that they name: `expert_ids`: A token's two ids in a layer differ. In the rows of one device in one layer (aligned blocks of 64 rows, layer by layer) some expert may be named by all 64 rows.
All inputs are finite; a program needn't handle non-finite values.
Results may differ from the reference program's by a relative error of at most 0.014.
Values may be sent and summed in bfloat16 or wider, within the bound.
A program may use at most 128 MiB of HBM per device.

```python
import math
import jax
import jax.numpy as jnp
import numpy as np
from jax import lax

D = 4096
FF = 7168
LAYERS = 2
TOK_DEV = 64
EXPERTS = 4
TOKENS = 512
N_MP = 16


def draw_exit_layer(key, part):
    own_key = jax.random.fold_in(key, 17)
    key_roll, key_early = jax.random.split(own_key)
    roll_value = jax.random.randint(key_roll, (TOKENS,), 0, 100)
    early_exit = jax.random.randint(key_early, (TOKENS,), 1, max(LAYERS, 2))
    exits = jnp.where(roll_value < 95, LAYERS, early_exit)
    position = jnp.arange(TOKENS)
    exits = jnp.where(position == 0, 1, jnp.where(position == 1, LAYERS, exits))
    return exits.astype(jnp.int32)


def place_ends(array, stream_key, least, largest):
    place = [jax.random.randint(jax.random.fold_in(stream_key, axis), (), 0, length) for axis, length in enumerate(array.shape)]
    main_axis = array.shape.index(max(array.shape))
    beside = place[:main_axis] + [(place[main_axis] + 1) % array.shape[main_axis]] + place[main_axis + 1:]
    return array.at[tuple(place)].set(least).at[tuple(beside)].set(largest)


def shard_levels(rng, dims, cuts, smallest, high):
    def one(dim, parts):
        steps = jax.random.uniform(jax.random.fold_in(jax.random.fold_in(rng, 6), dim), (parts,), jnp.float32, smallest / len(cuts), high / len(cuts))
        return jnp.repeat(jnp.exp(steps), dims[dim] // parts).reshape((-1,) + (1,) * (len(dims) - dim - 1))

    loudness = one(*cuts[0])
    for cut in cuts[1:]:
        loudness = loudness * one(*cut)
    return loudness


def routed_block(key, own, number, rows, amount, top, limit, skew):
    order = jax.random.permutation(key, amount)
    packed, ordinary = portions_of(amount, rows * top, limit, skew, True), portions_of(amount, rows * top, limit, skew, False)
    places = jnp.arange(amount)

    def named(sizes, turn):
        used = int((sizes > 0).sum())
        fixed = max(1, used // 4)
        shifted = fixed + (places - fixed + turn * (used - fixed)) % max(1, amount - fixed)
        return jnp.zeros((amount,), jnp.int32).at[order[jnp.where(places < fixed, places, shifted)]].set(jnp.asarray(sizes, jnp.int32))

    sizes = jnp.where(number % 4 == 0, named(packed, number // 4), named(ordinary, number - number // 4 - 1))
    mixed = jax.random.permutation(jax.random.fold_in(own, 3), amount)
    source_of, taker = mixed[0:amount // 2 * 2:2], mixed[1:amount // 2 * 2:2]
    slack = jnp.minimum(sizes[source_of] - 1, limit - sizes[taker]) // 2
    slack = jnp.where((source_of == order[0]) | (taker == order[0]) | (sizes[taker] == 0), 0, jnp.maximum(slack, 0))
    shifted = jax.random.randint(jax.random.fold_in(own, 4), (amount // 2,), 0, 1 << 20) % (slack + 1)
    sizes = sizes.at[source_of].add(-shifted).at[taker].add(shifted)
    members = jnp.searchsorted(jnp.cumsum(sizes), jnp.arange(rows * top), side="right").astype(jnp.int32)
    table = members.reshape(top, rows).T
    table = table[jax.random.permutation(jax.random.fold_in(own, 1), rows)]
    turn = jax.random.randint(jax.random.fold_in(own, 2), (rows, 1), 0, top)
    return jnp.take_along_axis(table, (jnp.arange(top)[None, :] + turn) % top, axis=1)


def portions_of(count, total, reach, lean, full):
    portions = [(1 << 20) // math.isqrt(standing ** lean) + 1 for standing in range(1, count + 1)]
    largest = reach if full else min(reach, max(-(-total // count), total * portions[0] // sum(portions)))
    least = 1 if total - largest >= count - 1 else 0
    holding, surplus = [largest] + [least] * (count - 1), total - largest - least * (count - 1)
    while surplus > 0:
        free = [i for i in range(1, count) if holding[i] < largest] or [i for i in range(1, count) if holding[i] < reach]
        whole, left = sum([portions[i] for i in free]), surplus
        for i in free:
            more = min(reach - holding[i], max(1, left * portions[i] // whole), surplus)
            holding[i] = holding[i] + more
            surplus = surplus - more
    return np.array(holding)


def centred(key, shape, deviation, most, pieces=(), held_as=jnp.bfloat16):
    drawn = jax.random.normal(key, shape, jnp.float32) * deviation
    if len(pieces) > 0:
        drawn = shard_levels(key, shape, pieces, -0.22, 0.18) * drawn
    return jnp.clip(drawn, min=-most, max=most).astype(held_as)


def setup_inputs(seed: int = 0, part: int = 0) -> dict:
    key_of = jax.random.split(jax.random.key(seed), 9)
    own_keys = jax.random.split(jax.random.fold_in(key_of[8], part), 9)
    hidden_in = centred(own_keys[0], (TOKENS, D), 1.0, 6.0, ((0, 8), (1, 16)))
    norm_gain = jnp.clip(1.0 + 0.15 * jax.random.normal(key_of[1], (LAYERS, D), jnp.float32), 0.25, 1.75).astype(jnp.bfloat16)
    expert_ids_keys = jax.random.split(jax.random.fold_in(own_keys[2], 1), LAYERS * TOKENS // TOK_DEV)
    expert_ids_turns = jax.random.permutation(jax.random.fold_in(own_keys[2], 3), LAYERS * TOKENS // TOK_DEV)
    expert_ids = jax.vmap(lambda own, number: routed_block(jax.random.fold_in(own_keys[2], 2), own, number, TOK_DEV, EXPERTS, 2, TOK_DEV, 2))(expert_ids_keys, expert_ids_turns).reshape((LAYERS, TOKENS, 2))
    gate_counts = place_ends(jax.random.randint(own_keys[3], (LAYERS, TOKENS, 2), 8, 16), jax.random.fold_in(own_keys[3], 1), 8, 15).astype(jnp.int32)
    exit_layer = draw_exit_layer(jax.random.fold_in(jax.random.fold_in(key_of[8], part), 71), part)
    w_gate = centred(key_of[5], (LAYERS, EXPERTS, FF, D), D ** -0.5, 0.09375, ((1, 4), (2, 32)))
    w_up = centred(key_of[6], (LAYERS, EXPERTS, FF, D), D ** -0.5, 0.09375, ((1, 4), (2, 32)))
    w_down = centred(key_of[7], (LAYERS, EXPERTS, FF, D), FF ** -0.5, 0.0625, ((1, 4), (2, 32)))
    return {"hidden_in": hidden_in, "norm_gain": norm_gain, "expert_ids": expert_ids, "gate_counts": gate_counts, "exit_layer": exit_layer, "w_gate": w_gate, "w_up": w_up, "w_down": w_down}


norm_floor = 0.1

def expert_output(normed, gate_rows, up_rows, down_rows):
    contract = (((1,), (1,)), ((), ()))
    gate_val = lax.dot_general(normed, gate_rows, contract, preferred_element_type=jnp.float32)
    up_val = lax.dot_general(normed, up_rows, contract, preferred_element_type=jnp.float32)
    hidden = (jax.nn.silu(gate_val) * up_val).astype(jnp.bfloat16)
    block_len = FF // N_MP
    running = jnp.zeros((normed.shape[0], D), jnp.float32)
    for block_idx in range(N_MP):
        row_start = block_idx * block_len
        partial_value = jnp.dot(hidden[:, row_start:row_start + block_len], down_rows[row_start:row_start + block_len], preferred_element_type=jnp.float32)
        rounded = lax.optimization_barrier(partial_value.astype(jnp.bfloat16))
        running = running + rounded.astype(jnp.float32)
    return running.astype(jnp.bfloat16)

def reference(hidden_in, norm_gain, expert_ids, gate_counts, exit_layer, w_gate, w_up, w_down):
    current = hidden_in
    expert_range = jnp.arange(EXPERTS, dtype=jnp.int32)
    for layer_idx in range(LAYERS):
        current_f32 = current.astype(jnp.float32)
        sum_squares = lax.optimization_barrier(jnp.sum(current_f32 * current_f32, axis=1, keepdims=True))
        inv_rms = lax.rsqrt(sum_squares / D + norm_floor)
        normed = (current_f32 * inv_rms * norm_gain[layer_idx].astype(jnp.float32)[None, :]).astype(jnp.bfloat16)
        outputs = lax.map(lambda weights: expert_output(normed, weights[0], weights[1], weights[2]), (w_gate[layer_idx], w_up[layer_idx], w_down[layer_idx]))
        counts = gate_counts[layer_idx].astype(jnp.float32)
        gate_share = counts / lax.optimization_barrier(jnp.sum(counts, axis=1, keepdims=True))
        matched = expert_ids[layer_idx][:, :, None] == expert_range[None, None, :]
        weight_te = lax.optimization_barrier(jnp.sum(jnp.where(matched, gate_share[:, :, None], jnp.float32(0.0)), axis=1))
        active = (exit_layer > layer_idx).astype(jnp.float32)
        weight_te = weight_te * active[:, None]
        update = jnp.einsum('te,etd->td', weight_te, outputs.astype(jnp.float32), precision=lax.Precision.HIGHEST)
        current = (current_f32 + update).astype(jnp.bfloat16)
    return current
```

```python
import jax
import jax.numpy as jnp
from jax import lax
from jax.experimental import pallas as pl
from jax.experimental.pallas import tpu as pltpu
from jax.sharding import PartitionSpec as P

LAYERS = 2
NORM_FLOOR = 0.1
MESH = pl.DeviceIdType.MESH

ORDER = (0, 1, -1, 4, -4, 2, -2, 7, -7, 3, -3, 5, -5, 6, -6, 8)
HUBS = (7, -7, 4, -4, 1, -1)
FORWARD = {1: (1,), -1: (-1,), 4: (1, -1), -4: (-1, 1), 7: (1, -1), -7: (1,)}
LEAVES = tuple(h + s for h in HUBS for s in FORWARD[h])
TO_HUB = {h + s: -s for h in HUBS for s in FORWARD[h]}
AG_LAG = (3, 6)
RS_LAG = (3, 6)


def kernel(
    cur_in, gain_in, ids_in, counts_in, exit_in, wg_hbm, wu_hbm, wd_hbm, out_ref,
    acts, gains, routes, wgu, wdn, acc, ssq, hid, part, xa, xb, stage, zleaf, zdest,
    zr, xr, gr, rr, xas, xbs, zls, zds, lw, rw, sw, sends,
):
    m, e, d = lax.axis_index("mp"), lax.axis_index("expert"), lax.axis_index("dp")
    n_mp, n_x = acts.shape[1], acts.shape[2]
    rows, width = cur_in.shape
    half = rows // 2
    tokens = n_x * rows
    hidden = 2 * wdn.shape[2]
    full = n_mp * width

    def z(step):
        return {"mp": lax.rem(m + (step + n_mp), n_mp)}

    def x(step):
        return {"expert": lax.rem(e + (step + n_x), n_x)}

    partner = {"dp": 1 - d}
    em, ep, eo = (lax.rem(e + s, n_x) for s in (n_x - 1, 1, 2))

    def owner(delta):
        return lax.rem(m + (n_mp - delta), n_mp)

    def send(src, dst, ssem, rsem, dev):
        pltpu.make_async_remote_copy(
            src_ref=src, dst_ref=dst, send_sem=ssem, recv_sem=rsem, device_id=dev, device_id_type=MESH
        ).start()

    def await_bytes(ref, sem):
        pltpu.make_async_copy(ref, ref, sem).wait()

    def weight_parts(layer):
        return (
            (wg_hbm.at[layer, 0], lambda s: wgu.at[layer, 0, s], 0),
            (wu_hbm.at[layer, 0], lambda s: wgu.at[layer, 1, s], 1),
            (wd_hbm.at[layer, 0], lambda s: wdn.at[layer, s], 2),
        )

    def load_weights(layer):
        for src, dst, j in weight_parts(layer):
            pltpu.make_async_copy(src, dst(0), lw.at[layer, j]).start()

    def give_weights(layer):
        for src, dst, j in weight_parts(layer):
            send(src, dst(1), sw.at[layer, j], rw.at[layer, j], partner)

    load_weights(0)

    lines = []
    for layer in range(LAYERS):
        counts = counts_in[layer].astype(jnp.float32)
        share = counts / jnp.sum(counts, axis=0, keepdims=True)
        active = exit_in[...] > layer
        for expert in range(n_x):
            named = jnp.where((ids_in[layer] == expert) & active, share, 0.0)
            lines.append(jnp.sum(named, axis=0, keepdims=True))
    routes[e, :, 0:rows] = jnp.concatenate(lines, axis=0)
    routes[e, :, rows:] = jnp.zeros((LAYERS * n_x, routes.shape[2] - rows), jnp.float32)
    gains[m] = gain_in[...].astype(jnp.float32)
    acts[0, m, e] = cur_in[...]

    barrier = pltpu.get_barrier_semaphore()
    peers = [z(h) for h in HUBS] + [x(1), x(-1), x(2), partner]
    for dev in peers:
        pl.semaphore_signal(barrier, inc=1, device_id=dev, device_id_type=MESH)
    pl.semaphore_wait(barrier, len(peers))

    def layer_step(layer, carry):
        own = acts.at[layer, m, e]
        for h in HUBS:
            send(own, own, sends.at[0], zr.at[layer, ORDER.index(h)], z(h))

        def spread(i):
            block = acts.at[layer, owner(ORDER[i]), e]
            send(block, block, sends.at[1], xr.at[layer, i, 0], x(1))
            send(block, block, sends.at[1], xr.at[layer, i, 1], x(-1))

        spread(0)

        @pl.when(layer == 0)
        def _():
            for h in HUBS:
                send(gains.at[m], gains.at[m], sends.at[2], gr.at[ORDER.index(h)], z(h))
            for j, s in enumerate((1, -1, 2)):
                send(routes.at[e], routes.at[e], sends.at[3], rr.at[j], x(s))
            give_weights(0)

        def take_z(i):
            delta = ORDER[i]
            k = owner(delta)
            block = acts.at[layer, k, e]
            await_bytes(block, zr.at[layer, i])
            for s in FORWARD.get(delta, ()):
                send(block, block, sends.at[0], zr.at[layer, ORDER.index(delta + s)], z(s))
            spread(i)

            @pl.when(layer == 0)
            def _():
                await_bytes(gains.at[k], gr.at[i])
                for s in FORWARD.get(delta, ()):
                    send(gains.at[k], gains.at[k], sends.at[2], gr.at[ORDER.index(delta + s)], z(s))

        def take_x(i):
            k = owner(ORDER[i])
            lo, hi = acts.at[layer, k, em], acts.at[layer, k, ep]
            await_bytes(lo, xr.at[layer, i, 0])
            piece = acts.at[layer, k, em, pl.ds(0, half)]
            send(piece, piece, sends.at[1], xr.at[layer, i, 2], x(1))
            await_bytes(hi, xr.at[layer, i, 1])
            piece = acts.at[layer, k, ep, pl.ds(half, half)]
            send(piece, piece, sends.at[1], xr.at[layer, i, 2], x(-1))

        def multiply(i):
            k = owner(ORDER[i])
            await_bytes(acts.at[layer, k, eo], xr.at[layer, i, 2])
            block = acts[layer, k].reshape(tokens, width).astype(jnp.float32)
            squares = block * block
            scaled = (block * gains[k, pl.ds(layer, 1), :]).astype(jnp.bfloat16)
            at = pl.ds(pl.multiple_of(k * width, width), width)
            ssq[...] = squares if i == 0 else ssq[...] + squares

            def product(j, c):
                w = wgu[layer, j, :, :, at].reshape(hidden, width)
                p = lax.dot_general(scaled, w, (((1,), (1,)), ((), ())), preferred_element_type=jnp.float32)
                acc[j] = p if i == 0 else acc[j] + p
                return c

            lax.fori_loop(0, 2, product, 0)

        def weights_here(j):
            await_bytes(wdn.at[layer, 0], lw.at[layer, j])
            await_bytes(wdn.at[layer, 1], rw.at[layer, j])

        for t in range(n_mp + AG_LAG[1]):
            if 0 < t < n_mp:
                take_z(t)
            if 0 <= t - AG_LAG[0] < n_mp:
                take_x(t - AG_LAG[0])
            if 0 <= t - AG_LAG[1] < n_mp:
                if t == AG_LAG[1]:
                    weights_here(0)
                    weights_here(1)
                multiply(t - AG_LAG[1])

        @pl.when(layer == 0)
        def _():
            for j, s in enumerate((em, ep, eo)):
                await_bytes(routes.at[s], rr.at[j])
            load_weights(1)
            give_weights(1)

        eye = lax.broadcasted_iota(jnp.int32, (rows, rows), 0) == lax.broadcasted_iota(jnp.int32, (rows, rows), 1)
        columns = []
        for s in range(n_x):
            line = routes[s, pl.ds(layer * n_x + e, 1), 0:rows]
            columns.append(jnp.sum(jnp.where(eye, line, 0.0), axis=1, keepdims=True))
        weight = jnp.concatenate(columns, axis=0)
        inv = lax.rsqrt(jnp.sum(ssq[...], axis=1, keepdims=True) / full + NORM_FLOOR)
        gate = acc[0] * inv
        hid[...] = (gate / (1.0 + jnp.exp(-gate)) * (acc[1] * inv) * weight).astype(jnp.bfloat16)
        weights_here(2)

        def down(i):
            f = owner(ORDER[i])
            at = pl.ds(pl.multiple_of(f * width, width), width)
            w = wdn[layer, :, :, at].reshape(hidden, width)
            p = jnp.dot(hid[...], w, preferred_element_type=jnp.float32)
            part[f] = p.astype(jnp.bfloat16).reshape(n_x, rows, width)
            send(part.at[f, eo, pl.ds(half, half)], xa.at[layer, i, 0], sends.at[4], xas.at[layer, i, 0], x(1))
            send(part.at[f, eo, pl.ds(0, half)], xa.at[layer, i, 1], sends.at[4], xas.at[layer, i, 1], x(-1))

        def merge_x(i):
            f = owner(ORDER[i])
            for side, (to, at, step) in enumerate(((ep, half, 1), (em, 0, -1))):
                await_bytes(xa.at[layer, i, side], xas.at[layer, i, side])
                old = part[f, to, at : at + half, :].astype(jnp.float32)
                new = old + xa[layer, i, side].astype(jnp.float32)
                part[f, to, at : at + half, :] = new.astype(jnp.bfloat16)
                send(part.at[f, to], xb.at[layer, i, side], sends.at[4], xbs.at[layer, i, side], x(step))

        def merge_z(i):
            delta = ORDER[i]
            f = owner(delta)
            for side in range(2):
                await_bytes(xb.at[layer, i, side], xbs.at[layer, i, side])
            total = part[f, e].astype(jnp.float32)
            for side in range(2):
                total = total + xb[layer, i, side].astype(jnp.float32)
            if delta == 0:
                for j in range(len(HUBS)):
                    await_bytes(zdest.at[layer, j], zds.at[layer, j])
                    total = total + zdest[layer, j].astype(jnp.float32)
                new = (acts[layer, m, e].astype(jnp.float32) + total).astype(jnp.bfloat16)
                out_ref[...] = new

                @pl.when(layer == 0)
                def _():
                    acts[1, m, e] = new

                return
            for s in FORWARD.get(delta, ()):
                j = LEAVES.index(delta + s)
                await_bytes(zleaf.at[layer, j], zls.at[layer, j])
                total = total + zleaf[layer, j].astype(jnp.float32)
            stage[i] = total.astype(jnp.bfloat16)
            if delta in HUBS:
                j = HUBS.index(delta)
                send(stage.at[i], zdest.at[layer, j], sends.at[5], zds.at[layer, j], z(-delta))
            else:
                j = LEAVES.index(delta)
                send(stage.at[i], zleaf.at[layer, j], sends.at[5], zls.at[layer, j], z(TO_HUB[delta]))

        last = n_mp - 1
        for t in range(n_mp + RS_LAG[1]):
            if t < n_mp:
                down(last - t)
            if 0 <= t - RS_LAG[0] < n_mp:
                merge_x(last - (t - RS_LAG[0]))
            if 0 <= t - RS_LAG[1] < n_mp:
                merge_z(last - (t - RS_LAG[1]))

        some = acts.at[layer, pl.ds(0, n_mp - 1), pl.ds(0, 1)]
        most = acts.at[layer, :, pl.ds(0, 3)]
        await_bytes(some, sends.at[0])
        await_bytes(most, sends.at[1])
        await_bytes(most, sends.at[4])
        await_bytes(some, sends.at[5])
        return carry

    lax.fori_loop(0, LAYERS, layer_step, 0)
    await_bytes(gains.at[pl.ds(0, n_mp - 1)], sends.at[2])
    await_bytes(routes.at[pl.ds(0, n_x - 1)], sends.at[3])
    for layer in range(LAYERS):
        for j in range(3):
            await_bytes(wdn.at[layer, 1], sw.at[layer, j])


def solution(mesh):
    n_mp, n_x = mesh.shape["mp"], mesh.shape["expert"]

    def body(hidden_in, norm_gain, expert_ids, gate_counts, exit_layer, w_gate, w_up, w_down):
        rows, width = hidden_in.shape
        _, _, rank, full = w_gate.shape
        tokens, bf = n_x * rows, jnp.bfloat16
        vm, dma = pltpu.VMEM, pltpu.SemaphoreType.DMA
        vmem = pl.BlockSpec(memory_space=pltpu.VMEM)
        hbm = pl.BlockSpec(memory_space=pl.ANY)
        return pl.pallas_call(
            kernel,
            out_shape=jax.ShapeDtypeStruct((rows, width), bf),
            in_specs=[vmem] * 5 + [hbm] * 3,
            out_specs=vmem,
            scratch_shapes=[
                vm((LAYERS, n_mp, n_x, rows, width), bf),
                vm((n_mp, LAYERS, width), jnp.float32),
                vm((n_x, LAYERS * n_x, 128), jnp.float32),
                vm((LAYERS, 2, 2, rank, full), bf),
                vm((LAYERS, 2, rank, full), bf),
                vm((2, tokens, 2 * rank), jnp.float32),
                vm((tokens, width), jnp.float32),
                vm((tokens, 2 * rank), bf),
                vm((n_mp, n_x, rows, width), bf),
                vm((LAYERS, n_mp, 2, rows // 2, width), bf),
                vm((LAYERS, n_mp, 2, rows, width), bf),
                vm((n_mp, rows, width), bf),
                vm((LAYERS, len(LEAVES), rows, width), bf),
                vm((LAYERS, len(HUBS), rows, width), bf),
                dma((LAYERS, n_mp)),
                dma((LAYERS, n_mp, 3)),
                dma((n_mp,)),
                dma((3,)),
                dma((LAYERS, n_mp, 2)),
                dma((LAYERS, n_mp, 2)),
                dma((LAYERS, len(LEAVES))),
                dma((LAYERS, len(HUBS))),
                dma((LAYERS, 3)),
                dma((LAYERS, 3)),
                dma((LAYERS, 3)),
                dma((6,)),
            ],
            compiler_params=pltpu.CompilerParams(
                collective_id=0, has_side_effects=True, vmem_limit_bytes=60 * 1024 * 1024
            ),
        )(
            hidden_in,
            norm_gain,
            jnp.transpose(expert_ids, (0, 2, 1)),
            jnp.transpose(gate_counts, (0, 2, 1)),
            exit_layer[None, :],
            w_gate,
            w_up,
            w_down,
        )

    in_specs = (
        P(("groups", "expert", "dp"), "mp"),
        P(None, "mp"),
        P(None, ("groups", "expert", "dp"), None),
        P(None, ("groups", "expert", "dp"), None),
        P(("groups", "expert", "dp")),
        P(None, "expert", ("mp", "dp"), None),
        P(None, "expert", ("mp", "dp"), None),
        P(None, "expert", ("mp", "dp"), None),
    )
    out_specs = P(("groups", "expert", "dp"), "mp")
    return jax.shard_map(body, mesh=mesh, in_specs=in_specs, out_specs=out_specs, check_vma=False)
```

```python
import jax
import jax.numpy as jnp
from jax import lax
from jax.experimental import pallas as pl
from jax.experimental.pallas import tpu as pltpu
from jax.sharding import PartitionSpec as P

LAYERS = 2
NORM_FLOOR = 0.1
MESH = pl.DeviceIdType.MESH

CHILDREN = {
    0: ((4, False), (-4, False), (1, False), (-1, False)),
    1: ((2, True),),
    -1: ((-2, True),),
    4: ((7, False), (5, False), (3, True)),
    -4: ((-7, False), (-5, False), (-3, True)),
    7: ((8, False), (6, False)),
    -7: ((-6, False),),
}
PARENT = {c: p for p, cs in CHILDREN.items() for c, _ in cs}
SINGLE = tuple(c for cs in CHILDREN.values() for c, whole in cs if not whole)
WHOLE = tuple(c for cs in CHILDREN.values() for c, whole in cs if whole)
ORDER = (0, *PARENT)
STEPS = tuple(sorted({c - p for c, p in PARENT.items()} | {p - c for c, p in PARENT.items()}))


def plan():
    arrival = {0: 0.0, 1: 2.6, 4: 4.5, 5: 7.2, 7: 8.2, 6: 10.8, 8: 10.9}
    arrival |= {-d: t + 0.1 for d, t in arrival.items() if d not in (0, 8)}
    ops, start, done = [], -1.0, {}
    for delta in sorted(arrival, key=arrival.get):
        start = max(arrival[delta], start + 0.85)
        done[delta] = start + 5.6
        ops += [(arrival[delta], "z", delta), (start + 2.8, "x", delta), (done[delta], "m", delta)]
    ops += [(done[PARENT[delta]] + 3.6, "m", delta) for delta in WHOLE]
    return [(kind, delta) for _, kind, delta in sorted(ops)]


PLAN = plan()


def kernel(
    cur_in, gain_in, ids_in, counts_in, exit_in, wg_hbm, wu_hbm, wd_hbm, out_ref,
    acts, gains, routes, wgu, wdn, acc, ssq, hid, part, xa, xb, stage, zin, zrow,
    zr, xr, gr, rr, xas, xbs, zs, zrs, lw, rw, sw, sends,
):
    m, e, d = lax.axis_index("mp"), lax.axis_index("expert"), lax.axis_index("dp")
    n_mp, n_x = acts.shape[1], acts.shape[2]
    rows, width = cur_in.shape
    half = rows // 2
    tokens = n_x * rows
    hidden = 2 * wdn.shape[2]
    full = n_mp * width

    def z(step):
        return {"mp": lax.rem(m + (step + n_mp), n_mp)}

    def x(step):
        return {"expert": lax.rem(e + (step + n_x), n_x)}

    partner = {"dp": 1 - d}
    em, ep, eo = (lax.rem(e + s, n_x) for s in (n_x - 1, 1, 2))

    def owner(delta):
        return lax.rem(m + (n_mp - delta), n_mp)

    def send(src, dst, ssem, rsem, dev):
        pltpu.make_async_remote_copy(
            src_ref=src, dst_ref=dst, send_sem=ssem, recv_sem=rsem, device_id=dev, device_id_type=MESH
        ).start()

    def await_bytes(ref, sem):
        pltpu.make_async_copy(ref, ref, sem).wait()

    def weight_parts(layer):
        return (
            (wg_hbm.at[layer, 0], lambda s: wgu.at[layer, 0, s], 0),
            (wu_hbm.at[layer, 0], lambda s: wgu.at[layer, 1, s], 1),
            (wd_hbm.at[layer, 0], lambda s: wdn.at[layer, s], 2),
        )

    def load_weights(layer):
        for src, dst, j in weight_parts(layer):
            pltpu.make_async_copy(src, dst(0), lw.at[layer, j]).start()

    def give_weights(layer):
        for src, dst, j in weight_parts(layer):
            send(src, dst(1), sw.at[layer, j], rw.at[layer, j], partner)

    load_weights(0)

    lines = []
    for layer in range(LAYERS):
        counts = counts_in[layer].astype(jnp.float32)
        share = counts / jnp.sum(counts, axis=0, keepdims=True)
        active = exit_in[...] > layer
        for expert in range(n_x):
            named = jnp.where((ids_in[layer] == expert) & active, share, 0.0)
            lines.append(jnp.sum(named, axis=0, keepdims=True))
    routes[e, :, 0:rows] = jnp.concatenate(lines, axis=0)
    routes[e, :, rows:] = jnp.zeros((LAYERS * n_x, routes.shape[2] - rows), jnp.float32)
    gains[m] = gain_in[...].astype(jnp.float32)
    acts[0, m, e] = cur_in[...]

    barrier = pltpu.get_barrier_semaphore()
    peers = [z(h) for h in STEPS] + [x(1), x(-1), x(2), partner]
    for dev in peers:
        pl.semaphore_signal(barrier, inc=1, device_id=dev, device_id_type=MESH)
    pl.semaphore_wait(barrier, len(peers))

    def layer_step(layer, carry):
        def spread(delta):
            i = ORDER.index(delta)
            block = acts.at[layer, owner(delta), e]
            for child, whole in CHILDREN.get(delta, ()):
                if not whole:
                    send(block, block, sends.at[0], zr.at[layer, ORDER.index(child)], z(child - delta))
            send(block, block, sends.at[1], xr.at[layer, i, 0], x(1))
            send(block, block, sends.at[1], xr.at[layer, i, 1], x(-1))

            @pl.when(layer == 0)
            def _():
                gain = gains.at[owner(delta)]
                if delta != 0:
                    await_bytes(gain, gr.at[i])
                for child, _ in CHILDREN.get(delta, ()):
                    send(gain, gain, sends.at[2], gr.at[ORDER.index(child)], z(child - delta))

        def take_z(delta):
            if delta != 0:
                await_bytes(acts.at[layer, owner(delta), e], zr.at[layer, ORDER.index(delta)])
            spread(delta)
            if delta == 0:

                @pl.when(layer == 0)
                def _():
                    for j, s in enumerate((1, -1, 2)):
                        send(routes.at[e], routes.at[e], sends.at[3], rr.at[j], x(s))
                    give_weights(0)

        def take_x(delta):
            i, k = ORDER.index(delta), owner(delta)
            lo, hi = acts.at[layer, k, em], acts.at[layer, k, ep]
            await_bytes(lo, xr.at[layer, i, 0])
            piece = acts.at[layer, k, em, pl.ds(0, half)]
            send(piece, piece, sends.at[1], xr.at[layer, i, 2], x(1))
            await_bytes(hi, xr.at[layer, i, 1])
            piece = acts.at[layer, k, ep, pl.ds(half, half)]
            send(piece, piece, sends.at[1], xr.at[layer, i, 2], x(-1))

        def multiply(delta, first):
            i, k = ORDER.index(delta), owner(delta)
            row = acts.at[layer, k]
            if delta in WHOLE:
                await_bytes(row, zr.at[layer, i])

                @pl.when(layer == 0)
                def _():
                    await_bytes(gains.at[k], gr.at[i])

            else:
                await_bytes(acts.at[layer, k, eo], xr.at[layer, i, 2])
            for child, whole in CHILDREN.get(delta, ()):
                if whole:
                    send(row, row, sends.at[6], zr.at[layer, ORDER.index(child)], z(child - delta))
            block = acts[layer, k].reshape(tokens, width).astype(jnp.float32)
            squares = block * block
            scaled = (block * gains[k, pl.ds(layer, 1), :]).astype(jnp.bfloat16)
            at = pl.ds(pl.multiple_of(k * width, width), width)
            ssq[...] = squares if first else ssq[...] + squares

            def product(j, c):
                w = wgu[layer, j, :, :, at].reshape(hidden, width)
                p = lax.dot_general(scaled, w, (((1,), (1,)), ((), ())), preferred_element_type=jnp.float32)
                acc[j] = p if first else acc[j] + p
                return c

            lax.fori_loop(0, 2, product, 0)

        def weights_here(j):
            await_bytes(wdn.at[layer, 0], lw.at[layer, j])
            await_bytes(wdn.at[layer, 1], rw.at[layer, j])

        first = True
        for kind, delta in PLAN:
            if kind == "z":
                take_z(delta)
            elif kind == "x":
                take_x(delta)
            else:
                if first:
                    weights_here(0)
                    weights_here(1)
                multiply(delta, first)
                first = False

        @pl.when(layer == 0)
        def _():
            for j, s in enumerate((em, ep, eo)):
                await_bytes(routes.at[s], rr.at[j])
            load_weights(1)
            give_weights(1)

        eye = lax.broadcasted_iota(jnp.int32, (rows, rows), 0) == lax.broadcasted_iota(jnp.int32, (rows, rows), 1)
        columns = []
        for s in range(n_x):
            line = routes[s, pl.ds(layer * n_x + e, 1), 0:rows]
            columns.append(jnp.sum(jnp.where(eye, line, 0.0), axis=1, keepdims=True))
        weight = jnp.concatenate(columns, axis=0)
        inv = lax.rsqrt(jnp.sum(ssq[...], axis=1, keepdims=True) / full + NORM_FLOOR)
        gate = acc[0] * inv
        hid[...] = (gate / (1.0 + jnp.exp(-gate)) * (acc[1] * inv) * weight).astype(jnp.bfloat16)
        weights_here(2)

        def down(delta):
            i, f = ORDER.index(delta), owner(delta)
            at = pl.ds(pl.multiple_of(f * width, width), width)
            w = wdn[layer, :, :, at].reshape(hidden, width)
            p = jnp.dot(hid[...], w, preferred_element_type=jnp.float32)
            for child, whole in CHILDREN.get(delta, ()):
                if whole:
                    j = WHOLE.index(child)
                    await_bytes(zrow.at[layer, j], zrs.at[layer, j])
                    p = p + zrow[layer, j].reshape(tokens, width).astype(jnp.float32)
            part[f] = p.astype(jnp.bfloat16).reshape(n_x, rows, width)
            if delta in WHOLE:
                j = WHOLE.index(delta)
                send(part.at[f], zrow.at[layer, j], sends.at[7], zrs.at[layer, j], z(PARENT[delta] - delta))
                return
            send(part.at[f, eo, pl.ds(half, half)], xa.at[layer, i, 0], sends.at[4], xas.at[layer, i, 0], x(1))
            send(part.at[f, eo, pl.ds(0, half)], xa.at[layer, i, 1], sends.at[4], xas.at[layer, i, 1], x(-1))

        def merge_x(delta):
            i, f = ORDER.index(delta), owner(delta)
            for side, (to, at, step) in enumerate(((ep, half, 1), (em, 0, -1))):
                await_bytes(xa.at[layer, i, side], xas.at[layer, i, side])
                old = part[f, to, at : at + half, :].astype(jnp.float32)
                new = old + xa[layer, i, side].astype(jnp.float32)
                part[f, to, at : at + half, :] = new.astype(jnp.bfloat16)
                send(part.at[f, to], xb.at[layer, i, side], sends.at[4], xbs.at[layer, i, side], x(step))

        def merge_z(delta):
            i, f = ORDER.index(delta), owner(delta)
            for side in range(2):
                await_bytes(xb.at[layer, i, side], xbs.at[layer, i, side])
            total = part[f, e].astype(jnp.float32)
            for side in range(2):
                total = total + xb[layer, i, side].astype(jnp.float32)
            for child, whole in CHILDREN.get(delta, ()):
                if not whole:
                    j = SINGLE.index(child)
                    await_bytes(zin.at[layer, j], zs.at[layer, j])
                    total = total + zin[layer, j].astype(jnp.float32)
            if delta != 0:
                j = SINGLE.index(delta)
                stage[i] = total.astype(jnp.bfloat16)
                send(stage.at[i], zin.at[layer, j], sends.at[5], zs.at[layer, j], z(PARENT[delta] - delta))
                return
            new = (acts[layer, m, e].astype(jnp.float32) + total).astype(jnp.bfloat16)
            out_ref[...] = new

            @pl.when(layer == 0)
            def _():
                acts[1, m, e] = new

        for kind, delta in reversed(PLAN):
            if kind == "m":
                down(delta)
            elif kind == "x":
                merge_x(delta)
            else:
                merge_z(delta)

        singles = acts.at[layer, pl.ds(0, len(SINGLE)), pl.ds(0, 1)]
        threes = acts.at[layer, pl.ds(0, len(SINGLE) + 1), pl.ds(0, 3)]
        rows_of_four = acts.at[layer, pl.ds(0, len(WHOLE))]
        for j, sent in ((0, singles), (1, threes), (4, threes), (5, singles), (6, rows_of_four), (7, rows_of_four)):
            await_bytes(sent, sends.at[j])
        return carry

    lax.fori_loop(0, LAYERS, layer_step, 0)
    await_bytes(gains.at[pl.ds(0, n_mp - 1)], sends.at[2])
    await_bytes(routes.at[pl.ds(0, n_x - 1)], sends.at[3])
    for layer in range(LAYERS):
        for j in range(3):
            await_bytes(wdn.at[layer, 1], sw.at[layer, j])


def solution(mesh):
    n_mp, n_x = mesh.shape["mp"], mesh.shape["expert"]

    def body(hidden_in, norm_gain, expert_ids, gate_counts, exit_layer, w_gate, w_up, w_down):
        rows, width = hidden_in.shape
        _, _, rank, full = w_gate.shape
        tokens, bf = n_x * rows, jnp.bfloat16
        vm, dma = pltpu.VMEM, pltpu.SemaphoreType.DMA
        vmem = pl.BlockSpec(memory_space=pltpu.VMEM)
        hbm = pl.BlockSpec(memory_space=pl.ANY)
        return pl.pallas_call(
            kernel,
            out_shape=jax.ShapeDtypeStruct((rows, width), bf),
            in_specs=[vmem] * 5 + [hbm] * 3,
            out_specs=vmem,
            scratch_shapes=[
                vm((LAYERS, n_mp, n_x, rows, width), bf),
                vm((n_mp, LAYERS, width), jnp.float32),
                vm((n_x, LAYERS * n_x, 128), jnp.float32),
                vm((LAYERS, 2, 2, rank, full), bf),
                vm((LAYERS, 2, rank, full), bf),
                vm((2, tokens, 2 * rank), jnp.float32),
                vm((tokens, width), jnp.float32),
                vm((tokens, 2 * rank), bf),
                vm((n_mp, n_x, rows, width), bf),
                vm((LAYERS, n_mp, 2, rows // 2, width), bf),
                vm((LAYERS, n_mp, 2, rows, width), bf),
                vm((n_mp, rows, width), bf),
                vm((LAYERS, len(SINGLE), rows, width), bf),
                vm((LAYERS, len(WHOLE), n_x, rows, width), bf),
                dma((LAYERS, n_mp)),
                dma((LAYERS, n_mp, 3)),
                dma((n_mp,)),
                dma((3,)),
                dma((LAYERS, n_mp, 2)),
                dma((LAYERS, n_mp, 2)),
                dma((LAYERS, len(SINGLE))),
                dma((LAYERS, len(WHOLE))),
                dma((LAYERS, 3)),
                dma((LAYERS, 3)),
                dma((LAYERS, 3)),
                dma((8,)),
            ],
            compiler_params=pltpu.CompilerParams(
                collective_id=0, has_side_effects=True, vmem_limit_bytes=60 * 1024 * 1024
            ),
        )(
            hidden_in,
            norm_gain,
            jnp.transpose(expert_ids, (0, 2, 1)),
            jnp.transpose(gate_counts, (0, 2, 1)),
            exit_layer[None, :],
            w_gate,
            w_up,
            w_down,
        )

    in_specs = (
        P(("groups", "expert", "dp"), "mp"),
        P(None, "mp"),
        P(None, ("groups", "expert", "dp"), None),
        P(None, ("groups", "expert", "dp"), None),
        P(("groups", "expert", "dp")),
        P(None, "expert", ("mp", "dp"), None),
        P(None, "expert", ("mp", "dp"), None),
        P(None, "expert", ("mp", "dp"), None),
    )
    out_specs = P(("groups", "expert", "dp"), "mp")
    return jax.shard_map(body, mesh=mesh, in_specs=in_specs, out_specs=out_specs, check_vma=False)
```

```python
import jax
import jax.numpy as jnp
from jax import lax
from jax.experimental import pallas as pl
from jax.experimental.pallas import tpu as pltpu
from jax.sharding import PartitionSpec as P

LAYERS = 2
NORM_FLOOR = 0.1
MESH = pl.DeviceIdType.MESH

OUT = {4: (0, False), 6: (4, False), 1: (0, False), 7: (4, False), 8: (6, False), 2: (1, False), 3: (4, True), 5: (4, True)}
BACK = {4: (0, False), 8: (4, False), 3: (0, False), 7: (4, False), 6: (4, False), 1: (0, False), 2: (1, True), 5: (4, True)}
OUT_PLAN = (
    ("z", 0), ("x", 0), ("z", 4), ("z", -4), ("z", 1), ("z", -1), ("x", 4), ("z", 6), ("x", -4), ("m", 0), ("x", 1), ("z", -7),
    ("x", -1), ("z", -6), ("z", 7), ("m", 4), ("z", 2), ("m", -4), ("z", -2), ("z", 8), ("x", 6), ("x", -7), ("m", 1), ("x", 7),
    ("x", -6), ("x", 2), ("m", -1), ("x", -2), ("m", 3), ("x", 8), ("m", 5), ("m", 6), ("m", 7), ("m", -7), ("m", 2), ("m", -6),
    ("m", -3), ("m", -5), ("m", 8), ("m", -2),
)
BACK_PLAN = (
    ("m", 8), ("m", 5), ("m", -7), ("m", 7), ("m", -5), ("m", -6), ("m", -2), ("m", 6), ("m", 2), ("x", 8), ("m", 3), ("m", -3),
    ("m", 0), ("x", -7), ("x", 7), ("x", -6), ("x", 6), ("z", 8), ("m", 4), ("m", -4), ("x", -3), ("x", 3), ("x", 0), ("z", -7),
    ("m", 1), ("z", 7), ("m", -1), ("z", -6), ("x", 4), ("z", 6), ("x", -4), ("x", 1), ("z", 3), ("z", -3), ("x", -1), ("z", -4),
    ("z", 4), ("z", 1), ("z", -1), ("z", 0),
)


class Tree:
    def __init__(self, half):
        self.parent, self.whole = {}, []
        for delta, (parent, whole) in half.items():
            for sign in (1,) if delta == 8 else (1, -1):
                self.parent[sign * delta] = sign * parent
                if whole:
                    self.whole.append(sign * delta)
        self.single = [delta for delta in self.parent if delta not in self.whole]
        self.order = [0, *self.parent]

    def below(self, delta, whole):
        among = self.whole if whole else self.single
        return [c for c in among if self.parent[c] == delta]

    def steps(self):
        return {s * (c - p) for c, p in self.parent.items() for s in (1, -1)}


OUT, BACK = Tree(OUT), Tree(BACK)
STEPS = sorted(OUT.steps() | BACK.steps())


def kernel(
    cur_in, gain_in, ids_in, counts_in, exit_in, wg_hbm, wu_hbm, wd_hbm, out_ref,
    acts, gains, routes, wgu, wdn, acc, ssq, hid, part, xa, xb, stage, zin, zrow,
    zr, xr, gr, rr, xas, xbs, zs, zrs, lw, rw, sw, sends,
):
    m, e, d = lax.axis_index("mp"), lax.axis_index("expert"), lax.axis_index("dp")
    n_mp, n_x = acts.shape[1], acts.shape[2]
    rows, width = cur_in.shape
    half = rows // 2
    tokens = n_x * rows
    hidden = 2 * wdn.shape[2]
    full = n_mp * width

    def z(step):
        return {"mp": lax.rem(m + (step + n_mp), n_mp)}

    def x(step):
        return {"expert": lax.rem(e + (step + n_x), n_x)}

    partner = {"dp": 1 - d}
    em, ep, eo = (lax.rem(e + s, n_x) for s in (n_x - 1, 1, 2))

    def owner(delta):
        return lax.rem(m + (n_mp - delta), n_mp)

    def send(src, dst, ssem, rsem, dev):
        pltpu.make_async_remote_copy(
            src_ref=src, dst_ref=dst, send_sem=ssem, recv_sem=rsem, device_id=dev, device_id_type=MESH
        ).start()

    def await_bytes(ref, sem):
        pltpu.make_async_copy(ref, ref, sem).wait()

    def weight_parts(layer):
        return (
            (wg_hbm.at[layer, 0], lambda s: wgu.at[layer, 0, s], 0),
            (wu_hbm.at[layer, 0], lambda s: wgu.at[layer, 1, s], 1),
            (wd_hbm.at[layer, 0], lambda s: wdn.at[layer, s], 2),
        )

    def load_weights(layer):
        for src, dst, j in weight_parts(layer):
            pltpu.make_async_copy(src, dst(0), lw.at[layer, j]).start()

    def give_weights(layer):
        for src, dst, j in weight_parts(layer):
            send(src, dst(1), sw.at[layer, j], rw.at[layer, j], partner)

    load_weights(0)

    lines = []
    for layer in range(LAYERS):
        counts = counts_in[layer].astype(jnp.float32)
        share = counts / jnp.sum(counts, axis=0, keepdims=True)
        active = exit_in[...] > layer
        for expert in range(n_x):
            named = jnp.where((ids_in[layer] == expert) & active, share, 0.0)
            lines.append(jnp.sum(named, axis=0, keepdims=True))
    routes[e, :, 0:rows] = jnp.concatenate(lines, axis=0)
    routes[e, :, rows:] = jnp.zeros((LAYERS * n_x, routes.shape[2] - rows), jnp.float32)
    gains[m] = gain_in[...].astype(jnp.float32)
    acts[0, m, e] = cur_in[...]

    barrier = pltpu.get_barrier_semaphore()
    peers = [z(h) for h in STEPS] + [x(1), x(-1), x(2), partner]
    for dev in peers:
        pl.semaphore_signal(barrier, inc=1, device_id=dev, device_id_type=MESH)
    pl.semaphore_wait(barrier, len(peers))

    def layer_step(layer, carry):
        def spread(delta):
            i = OUT.order.index(delta)
            block = acts.at[layer, owner(delta), e]
            for child in OUT.below(delta, False):
                send(block, block, sends.at[0], zr.at[layer, OUT.order.index(child)], z(child - delta))
            send(block, block, sends.at[1], xr.at[layer, i, 0], x(1))
            send(block, block, sends.at[1], xr.at[layer, i, 1], x(-1))

            @pl.when(layer == 0)
            def _():
                gain = gains.at[owner(delta)]
                if delta != 0:
                    await_bytes(gain, gr.at[i])
                for child in OUT.below(delta, False) + OUT.below(delta, True):
                    send(gain, gain, sends.at[2], gr.at[OUT.order.index(child)], z(child - delta))

        def take_z(delta):
            if delta != 0:
                await_bytes(acts.at[layer, owner(delta), e], zr.at[layer, OUT.order.index(delta)])
            spread(delta)
            if delta == 0:

                @pl.when(layer == 0)
                def _():
                    for j, s in enumerate((1, -1, 2)):
                        send(routes.at[e], routes.at[e], sends.at[3], rr.at[j], x(s))
                    give_weights(0)

        def take_x(delta):
            i, k = OUT.order.index(delta), owner(delta)
            lo, hi = acts.at[layer, k, em], acts.at[layer, k, ep]
            await_bytes(lo, xr.at[layer, i, 0])
            piece = acts.at[layer, k, em, pl.ds(0, half)]
            send(piece, piece, sends.at[1], xr.at[layer, i, 2], x(1))
            await_bytes(hi, xr.at[layer, i, 1])
            piece = acts.at[layer, k, ep, pl.ds(half, half)]
            send(piece, piece, sends.at[1], xr.at[layer, i, 2], x(-1))

        def multiply(delta, first):
            i, k = OUT.order.index(delta), owner(delta)
            row = acts.at[layer, k]
            if delta in OUT.whole:
                await_bytes(row, zr.at[layer, i])

                @pl.when(layer == 0)
                def _():
                    await_bytes(gains.at[k], gr.at[i])

            else:
                await_bytes(acts.at[layer, k, eo], xr.at[layer, i, 2])
            for child in OUT.below(delta, True):
                send(row, row, sends.at[6], zr.at[layer, OUT.order.index(child)], z(child - delta))
            block = acts[layer, k].reshape(tokens, width).astype(jnp.float32)
            squares = block * block
            scaled = (block * gains[k, pl.ds(layer, 1), :]).astype(jnp.bfloat16)
            at = pl.ds(pl.multiple_of(k * width, width), width)
            ssq[...] = squares if first else ssq[...] + squares

            def product(j):
                w = wgu[layer, j, :, :, at].reshape(hidden, width)
                p = lax.dot_general(scaled, w, (((1,), (1,)), ((), ())), preferred_element_type=jnp.float32)
                acc[j] = p if first else acc[j] + p

            for j in range(2):
                product(j)

        def weights_here(j):
            await_bytes(wdn.at[layer, 0], lw.at[layer, j])
            await_bytes(wdn.at[layer, 1], rw.at[layer, j])

        first = True
        for kind, delta in OUT_PLAN:
            if kind == "z":
                take_z(delta)
            elif kind == "x":
                take_x(delta)
            else:
                if first:
                    weights_here(0)
                    weights_here(1)
                multiply(delta, first)
                first = False

        @pl.when(layer == 0)
        def _():
            for j, s in enumerate((em, ep, eo)):
                await_bytes(routes.at[s], rr.at[j])
            load_weights(1)
            give_weights(1)

        eye = lax.broadcasted_iota(jnp.int32, (rows, rows), 0) == lax.broadcasted_iota(jnp.int32, (rows, rows), 1)
        columns = []
        for s in range(n_x):
            line = routes[s, pl.ds(layer * n_x + e, 1), 0:rows]
            columns.append(jnp.sum(jnp.where(eye, line, 0.0), axis=1, keepdims=True))
        weight = jnp.concatenate(columns, axis=0)
        inv = lax.rsqrt(jnp.sum(ssq[...], axis=1, keepdims=True) / full + NORM_FLOOR)
        gate = acc[0] * inv
        hid[...] = (gate / (1.0 + jnp.exp(-gate)) * (acc[1] * inv) * weight).astype(jnp.bfloat16)
        weights_here(2)

        def down(delta):
            i, f = BACK.order.index(delta), owner(delta)
            at = pl.ds(pl.multiple_of(f * width, width), width)
            w = wdn[layer, :, :, at].reshape(hidden, width)
            p = jnp.dot(hid[...], w, preferred_element_type=jnp.float32)
            for child in BACK.below(delta, True):
                j = BACK.whole.index(child)
                await_bytes(zrow.at[layer, j], zrs.at[layer, j])
                p = p + zrow[layer, j].reshape(tokens, width).astype(jnp.float32)
            part[f] = p.astype(jnp.bfloat16).reshape(n_x, rows, width)
            if delta in BACK.whole:
                j = BACK.whole.index(delta)
                send(part.at[f], zrow.at[layer, j], sends.at[7], zrs.at[layer, j], z(BACK.parent[delta] - delta))
                return
            send(part.at[f, eo, pl.ds(half, half)], xa.at[layer, i, 0], sends.at[4], xas.at[layer, i, 0], x(1))
            send(part.at[f, eo, pl.ds(0, half)], xa.at[layer, i, 1], sends.at[4], xas.at[layer, i, 1], x(-1))

        def merge_x(delta):
            i, f = BACK.order.index(delta), owner(delta)
            for side, (to, at, step) in enumerate(((ep, half, 1), (em, 0, -1))):
                await_bytes(xa.at[layer, i, side], xas.at[layer, i, side])
                old = part[f, to, at : at + half, :].astype(jnp.float32)
                new = old + xa[layer, i, side].astype(jnp.float32)
                part[f, to, at : at + half, :] = new.astype(jnp.bfloat16)
                send(part.at[f, to], xb.at[layer, i, side], sends.at[4], xbs.at[layer, i, side], x(step))

        def merge_z(delta):
            i, f = BACK.order.index(delta), owner(delta)
            for side in range(2):
                await_bytes(xb.at[layer, i, side], xbs.at[layer, i, side])
            total = part[f, e].astype(jnp.float32)
            for side in range(2):
                total = total + xb[layer, i, side].astype(jnp.float32)
            for child in BACK.below(delta, False):
                j = BACK.single.index(child)
                await_bytes(zin.at[layer, j], zs.at[layer, j])
                total = total + zin[layer, j].astype(jnp.float32)
            if delta != 0:
                j = BACK.single.index(delta)
                stage[i] = total.astype(jnp.bfloat16)
                send(stage.at[i], zin.at[layer, j], sends.at[5], zs.at[layer, j], z(BACK.parent[delta] - delta))
                return
            new = (acts[layer, m, e].astype(jnp.float32) + total).astype(jnp.bfloat16)
            out_ref[...] = new

            @pl.when(layer == 0)
            def _():
                acts[1, m, e] = new

        for kind, delta in BACK_PLAN:
            if kind == "m":
                down(delta)
            elif kind == "x":
                merge_x(delta)
            else:
                merge_z(delta)

        for tree, at in ((OUT, (0, 1, 6)), (BACK, (5, 4, 7))):
            await_bytes(acts.at[layer, pl.ds(0, len(tree.single)), pl.ds(0, 1)], sends.at[at[0]])
            await_bytes(acts.at[layer, pl.ds(0, len(tree.single) + 1), pl.ds(0, 3)], sends.at[at[1]])
            await_bytes(acts.at[layer, pl.ds(0, len(tree.whole))], sends.at[at[2]])
        return carry

    lax.fori_loop(0, LAYERS, layer_step, 0)
    await_bytes(gains.at[pl.ds(0, n_mp - 1)], sends.at[2])
    await_bytes(routes.at[pl.ds(0, n_x - 1)], sends.at[3])
    for layer in range(LAYERS):
        for j in range(3):
            await_bytes(wdn.at[layer, 1], sw.at[layer, j])


def solution(mesh):
    n_mp, n_x = mesh.shape["mp"], mesh.shape["expert"]

    def body(hidden_in, norm_gain, expert_ids, gate_counts, exit_layer, w_gate, w_up, w_down):
        rows, width = hidden_in.shape
        _, _, rank, full = w_gate.shape
        tokens, bf = n_x * rows, jnp.bfloat16
        vm, dma = pltpu.VMEM, pltpu.SemaphoreType.DMA
        vmem = pl.BlockSpec(memory_space=pltpu.VMEM)
        hbm = pl.BlockSpec(memory_space=pl.ANY)
        return pl.pallas_call(
            kernel,
            out_shape=jax.ShapeDtypeStruct((rows, width), bf),
            in_specs=[vmem] * 5 + [hbm] * 3,
            out_specs=vmem,
            scratch_shapes=[
                vm((LAYERS, n_mp, n_x, rows, width), bf),
                vm((n_mp, LAYERS, width), jnp.float32),
                vm((n_x, LAYERS * n_x, 128), jnp.float32),
                vm((LAYERS, 2, 2, rank, full), bf),
                vm((LAYERS, 2, rank, full), bf),
                vm((2, tokens, 2 * rank), jnp.float32),
                vm((tokens, width), jnp.float32),
                vm((tokens, 2 * rank), bf),
                vm((n_mp, n_x, rows, width), bf),
                vm((LAYERS, n_mp, 2, rows // 2, width), bf),
                vm((LAYERS, n_mp, 2, rows, width), bf),
                vm((n_mp, rows, width), bf),
                vm((LAYERS, len(BACK.single), rows, width), bf),
                vm((LAYERS, len(BACK.whole), n_x, rows, width), bf),
                dma((LAYERS, n_mp)),
                dma((LAYERS, n_mp, 3)),
                dma((n_mp,)),
                dma((3,)),
                dma((LAYERS, n_mp, 2)),
                dma((LAYERS, n_mp, 2)),
                dma((LAYERS, len(BACK.single))),
                dma((LAYERS, len(BACK.whole))),
                dma((LAYERS, 3)),
                dma((LAYERS, 3)),
                dma((LAYERS, 3)),
                dma((8,)),
            ],
            compiler_params=pltpu.CompilerParams(
                collective_id=0, has_side_effects=True, vmem_limit_bytes=60 * 1024 * 1024
            ),
        )(
            hidden_in,
            norm_gain,
            jnp.transpose(expert_ids, (0, 2, 1)),
            jnp.transpose(gate_counts, (0, 2, 1)),
            exit_layer[None, :],
            w_gate,
            w_up,
            w_down,
        )

    in_specs = (
        P(("groups", "expert", "dp"), "mp"),
        P(None, "mp"),
        P(None, ("groups", "expert", "dp"), None),
        P(None, ("groups", "expert", "dp"), None),
        P(("groups", "expert", "dp")),
        P(None, "expert", ("mp", "dp"), None),
        P(None, "expert", ("mp", "dp"), None),
        P(None, "expert", ("mp", "dp"), None),
    )
    out_specs = P(("groups", "expert", "dp"), "mp")
    return jax.shard_map(body, mesh=mesh, in_specs=in_specs, out_specs=out_specs, check_vma=False)
```

```python
import jax
import jax.numpy as jnp
from jax import lax
from jax.experimental import pallas as pl
from jax.experimental.pallas import tpu as pltpu
from jax.sharding import PartitionSpec as P

LAYERS = 2
NORM_FLOOR = 0.1
MESH = pl.DeviceIdType.MESH

OUT = {4: (0, False), 6: (4, False), 2: (0, False), 8: (6, False), 1: (0, True), 3: (4, True), 5: (4, True), 7: (6, False)}
BACK = {4: (0, False), 8: (4, False), 3: (0, False), 7: (4, False), 6: (4, False), 1: (0, False), 2: (1, True), 5: (4, True)}
OUT_DIRECT = (4, 6, 7, 8)
BACK_DIRECT = (1, 4, 6, 7, 8)
OUT_PLAN = (
    ("z", 0), ("x", 0), ("z", 4), ("z", -4), ("m", 0), ("z", 2), ("z", -2), ("z", 6), ("z", -6), ("m", 4), ("x", 2), ("x", -2),
    ("m", -4), ("m", 1), ("m", -1), ("z", -7), ("z", 8), ("z", 7), ("m", -2), ("m", 2), ("m", -6), ("m", 3), ("m", 6), ("m", 5),
    ("m", -7), ("m", 8), ("m", -5), ("m", -3), ("m", 7),
)
BACK_PLAN = (
    ("m", 8), ("m", 5), ("m", -5), ("m", -7), ("m", 2), ("m", -3), ("m", 7), ("m", -2), ("m", 3), ("m", -6), ("m", 6), ("z", 8),
    ("x", -3), ("m", 0), ("z", -7), ("x", 3), ("m", -4), ("z", 7), ("m", 4), ("z", -6), ("z", 6), ("m", -1), ("m", 1), ("z", -3),
    ("z", 3), ("z", 4), ("z", -4), ("x", 0), ("z", 1), ("z", -1), ("z", 0),
)


class Tree:
    def __init__(self, half):
        self.parent, self.whole = {}, []
        for delta, (parent, whole) in half.items():
            for sign in (1,) if delta == 8 else (1, -1):
                self.parent[sign * delta] = sign * parent
                if whole:
                    self.whole.append(sign * delta)
        self.single = [delta for delta in self.parent if delta not in self.whole]
        self.order = [0, *self.parent]

    def below(self, delta, whole):
        among = self.whole if whole else self.single
        return [c for c in among if self.parent[c] == delta]

    def steps(self):
        return {s * (c - p) for c, p in self.parent.items() for s in (1, -1)}


OUT, BACK = Tree(OUT), Tree(BACK)
STEPS = sorted(OUT.steps() | BACK.steps())


def kernel(
    cur_in, gain_in, ids_in, counts_in, exit_in, wg_hbm, wu_hbm, wd_hbm, out_ref,
    acts, gains, routes, wgu, wdn, acc, ssq, hid, part, xa, xb, xc, stage, zin, zrow,
    zr, xr, gr, rr, xas, xbs, zs, zrs, lw, rw, sw, sends,
):
    m, e, d = lax.axis_index("mp"), lax.axis_index("expert"), lax.axis_index("dp")
    n_mp, n_x = acts.shape[1], acts.shape[2]
    rows, width = cur_in.shape
    half = rows // 2
    tokens = n_x * rows
    hidden = 2 * wdn.shape[2]
    full = n_mp * width

    def z(step):
        return {"mp": lax.rem(m + (step + n_mp), n_mp)}

    def x(step):
        return {"expert": lax.rem(e + (step + n_x), n_x)}

    partner = {"dp": 1 - d}
    em, ep, eo = (lax.rem(e + s, n_x) for s in (n_x - 1, 1, 2))

    def owner(delta):
        return lax.rem(m + (n_mp - delta), n_mp)

    def send(src, dst, ssem, rsem, dev):
        pltpu.make_async_remote_copy(
            src_ref=src, dst_ref=dst, send_sem=ssem, recv_sem=rsem, device_id=dev, device_id_type=MESH
        ).start()

    def await_bytes(ref, sem):
        pltpu.make_async_copy(ref, ref, sem).wait()

    def weight_parts(layer):
        return (
            (wg_hbm.at[layer, 0], lambda s: wgu.at[layer, 0, s], 0),
            (wu_hbm.at[layer, 0], lambda s: wgu.at[layer, 1, s], 1),
            (wd_hbm.at[layer, 0], lambda s: wdn.at[layer, s], 2),
        )

    def load_weights(layer):
        for src, dst, j in weight_parts(layer):
            pltpu.make_async_copy(src, dst(0), lw.at[layer, j]).start()

    def give_weights(layer):
        for src, dst, j in weight_parts(layer):
            send(src, dst(1), sw.at[layer, j], rw.at[layer, j], partner)

    barrier = pltpu.get_barrier_semaphore()
    peers = [z(h) for h in STEPS] + [x(1), x(-1), x(2), partner]
    for dev in peers:
        pl.semaphore_signal(barrier, inc=1, device_id=dev, device_id_type=MESH)
    load_weights(0)

    lines = []
    for layer in range(LAYERS):
        counts = counts_in[layer].astype(jnp.float32)
        share = counts / jnp.sum(counts, axis=0, keepdims=True)
        active = exit_in[...] > layer
        for expert in range(n_x):
            named = jnp.where((ids_in[layer] == expert) & active, share, 0.0)
            lines.append(jnp.sum(named, axis=0, keepdims=True))
    routes[e, :, 0:rows] = jnp.concatenate(lines, axis=0)
    routes[e, :, rows:] = jnp.zeros((LAYERS * n_x, routes.shape[2] - rows), jnp.float32)
    gains[m] = gain_in[...].astype(jnp.float32)
    acts[0, m, e] = cur_in[...]

    pl.semaphore_wait(barrier, len(peers))

    def layer_step(layer, carry):
        def spread(delta):
            i = OUT.order.index(delta)
            block = acts.at[layer, owner(delta), e]
            for child in OUT.below(delta, False):
                send(block, block, sends.at[0], zr.at[layer, OUT.order.index(child)], z(child - delta))
            send(block, block, sends.at[1], xr.at[layer, i, 0], x(1))
            send(block, block, sends.at[1], xr.at[layer, i, 1], x(-1))
            if abs(delta) in OUT_DIRECT:
                send(block, block, sends.at[1], xr.at[layer, i, 2], x(2))

            @pl.when(layer == 0)
            def _():
                gain = gains.at[owner(delta)]
                if delta != 0:
                    await_bytes(gain, gr.at[i])
                for child in OUT.below(delta, False) + OUT.below(delta, True):
                    send(gain, gain, sends.at[2], gr.at[OUT.order.index(child)], z(child - delta))

        def take_z(delta):
            if delta != 0:
                await_bytes(acts.at[layer, owner(delta), e], zr.at[layer, OUT.order.index(delta)])
            spread(delta)
            if delta == 0:

                @pl.when(layer == 0)
                def _():
                    for j, s in enumerate((1, -1, 2)):
                        send(routes.at[e], routes.at[e], sends.at[3], rr.at[j], x(s))
                    give_weights(0)

        def take_x(delta):
            i, k = OUT.order.index(delta), owner(delta)
            lo, hi = acts.at[layer, k, em], acts.at[layer, k, ep]
            await_bytes(lo, xr.at[layer, i, 0])
            piece = acts.at[layer, k, em, pl.ds(0, half)]
            send(piece, piece, sends.at[1], xr.at[layer, i, 2], x(1))
            await_bytes(hi, xr.at[layer, i, 1])
            piece = acts.at[layer, k, ep, pl.ds(half, half)]
            send(piece, piece, sends.at[1], xr.at[layer, i, 2], x(-1))

        def multiply(delta, first):
            i, k = OUT.order.index(delta), owner(delta)
            row = acts.at[layer, k]
            if delta in OUT.whole:
                await_bytes(row, zr.at[layer, i])

                @pl.when(layer == 0)
                def _():
                    await_bytes(gains.at[k], gr.at[i])

            else:
                if abs(delta) in OUT_DIRECT:
                    await_bytes(acts.at[layer, k, em], xr.at[layer, i, 0])
                    await_bytes(acts.at[layer, k, ep], xr.at[layer, i, 1])
                await_bytes(acts.at[layer, k, eo], xr.at[layer, i, 2])
            for child in OUT.below(delta, True):
                send(row, row, sends.at[6], zr.at[layer, OUT.order.index(child)], z(child - delta))
            block = acts[layer, k].reshape(tokens, width).astype(jnp.float32)
            squares = block * block
            scaled = (block * gains[k, pl.ds(layer, 1), :]).astype(jnp.bfloat16)
            at = pl.ds(pl.multiple_of(k * width, width), width)
            ssq[...] = squares if first else ssq[...] + squares

            def product(j):
                w = wgu[layer, j, :, :, at].reshape(hidden, width)
                p = lax.dot_general(scaled, w, (((1,), (1,)), ((), ())), preferred_element_type=jnp.float32)
                acc[j] = p if first else acc[j] + p

            for j in range(2):
                product(j)

        def weights_here(j):
            await_bytes(wdn.at[layer, 0], lw.at[layer, j])
            await_bytes(wdn.at[layer, 1], rw.at[layer, j])

        first = True
        for kind, delta in OUT_PLAN:
            if kind == "z":
                take_z(delta)
            elif kind == "x":
                take_x(delta)
            else:
                if first:
                    weights_here(0)
                    weights_here(1)
                multiply(delta, first)
                first = False

        @pl.when(layer == 0)
        def _():
            for j, s in enumerate((em, ep, eo)):
                await_bytes(routes.at[s], rr.at[j])
            load_weights(1)
            give_weights(1)

        eye = lax.broadcasted_iota(jnp.int32, (rows, rows), 0) == lax.broadcasted_iota(jnp.int32, (rows, rows), 1)
        columns = []
        for s in range(n_x):
            line = routes[s, pl.ds(layer * n_x + e, 1), 0:rows]
            columns.append(jnp.sum(jnp.where(eye, line, 0.0), axis=1, keepdims=True))
        weight = jnp.concatenate(columns, axis=0)
        inv = lax.rsqrt(jnp.sum(ssq[...], axis=1, keepdims=True) / full + NORM_FLOOR)
        gate = acc[0] * inv
        hid[...] = (gate / (1.0 + jnp.exp(-gate)) * (acc[1] * inv) * weight).astype(jnp.bfloat16)
        weights_here(2)

        def down(delta):
            i, f = BACK.order.index(delta), owner(delta)
            at = pl.ds(pl.multiple_of(f * width, width), width)
            w = wdn[layer, :, :, at].reshape(hidden, width)
            p = jnp.dot(hid[...], w, preferred_element_type=jnp.float32)
            for child in BACK.below(delta, True):
                j = BACK.whole.index(child)
                await_bytes(zrow.at[layer, j], zrs.at[layer, j])
                p = p + zrow[layer, j].reshape(tokens, width).astype(jnp.float32)
            part[f] = p.astype(jnp.bfloat16).reshape(n_x, rows, width)
            if delta in BACK.whole:
                j = BACK.whole.index(delta)
                send(part.at[f], zrow.at[layer, j], sends.at[7], zrs.at[layer, j], z(BACK.parent[delta] - delta))
                return
            if abs(delta) in BACK_DIRECT:
                send(part.at[f, eo], xc.at[layer, i], sends.at[4], xas.at[layer, i, 0], x(2))
                send(part.at[f, ep], xb.at[layer, i, 0], sends.at[4], xbs.at[layer, i, 0], x(1))
                send(part.at[f, em], xb.at[layer, i, 1], sends.at[4], xbs.at[layer, i, 1], x(-1))
                return
            send(part.at[f, eo, pl.ds(half, half)], xa.at[layer, i, 0], sends.at[4], xas.at[layer, i, 0], x(1))
            send(part.at[f, eo, pl.ds(0, half)], xa.at[layer, i, 1], sends.at[4], xas.at[layer, i, 1], x(-1))

        def merge_x(delta):
            i, f = BACK.order.index(delta), owner(delta)
            for side, (to, at, step) in enumerate(((ep, half, 1), (em, 0, -1))):
                await_bytes(xa.at[layer, i, side], xas.at[layer, i, side])
                old = part[f, to, at : at + half, :].astype(jnp.float32)
                new = old + xa[layer, i, side].astype(jnp.float32)
                part[f, to, at : at + half, :] = new.astype(jnp.bfloat16)
                send(part.at[f, to], xb.at[layer, i, side], sends.at[4], xbs.at[layer, i, side], x(step))

        def merge_z(delta):
            i, f = BACK.order.index(delta), owner(delta)
            for side in range(2):
                await_bytes(xb.at[layer, i, side], xbs.at[layer, i, side])
            total = part[f, e].astype(jnp.float32)
            for side in range(2):
                total = total + xb[layer, i, side].astype(jnp.float32)
            if abs(delta) in BACK_DIRECT:
                await_bytes(xc.at[layer, i], xas.at[layer, i, 0])
                total = total + xc[layer, i].astype(jnp.float32)
            for child in BACK.below(delta, False):
                j = BACK.single.index(child)
                await_bytes(zin.at[layer, j], zs.at[layer, j])
                total = total + zin[layer, j].astype(jnp.float32)
            if delta != 0:
                j = BACK.single.index(delta)
                stage[i] = total.astype(jnp.bfloat16)
                send(stage.at[i], zin.at[layer, j], sends.at[5], zs.at[layer, j], z(BACK.parent[delta] - delta))
                return
            new = (acts[layer, m, e].astype(jnp.float32) + total).astype(jnp.bfloat16)
            out_ref[...] = new

            @pl.when(layer == 0)
            def _():
                acts[1, m, e] = new

        for kind, delta in BACK_PLAN:
            if kind == "m":
                down(delta)
            elif kind == "x":
                merge_x(delta)
            else:
                merge_z(delta)

        for tree, at in ((OUT, (0, 1, 6)), (BACK, (5, 4, 7))):
            await_bytes(acts.at[layer, pl.ds(0, len(tree.single)), pl.ds(0, 1)], sends.at[at[0]])
            await_bytes(acts.at[layer, pl.ds(0, len(tree.single) + 1), pl.ds(0, 3)], sends.at[at[1]])
            await_bytes(acts.at[layer, pl.ds(0, len(tree.whole))], sends.at[at[2]])
        return carry

    lax.fori_loop(0, LAYERS, layer_step, 0)
    await_bytes(gains.at[pl.ds(0, n_mp - 1)], sends.at[2])
    await_bytes(routes.at[pl.ds(0, n_x - 1)], sends.at[3])
    for layer in range(LAYERS):
        for j in range(3):
            await_bytes(wdn.at[layer, 1], sw.at[layer, j])


def solution(mesh):
    n_mp, n_x = mesh.shape["mp"], mesh.shape["expert"]

    def body(hidden_in, norm_gain, expert_ids, gate_counts, exit_layer, w_gate, w_up, w_down):
        rows, width = hidden_in.shape
        _, _, rank, full = w_gate.shape
        tokens, bf = n_x * rows, jnp.bfloat16
        vm, dma = pltpu.VMEM, pltpu.SemaphoreType.DMA
        vmem = pl.BlockSpec(memory_space=pltpu.VMEM)
        hbm = pl.BlockSpec(memory_space=pl.ANY)
        return pl.pallas_call(
            kernel,
            out_shape=jax.ShapeDtypeStruct((rows, width), bf),
            in_specs=[vmem] * 5 + [hbm] * 3,
            out_specs=vmem,
            scratch_shapes=[
                vm((LAYERS, n_mp, n_x, rows, width), bf),
                vm((n_mp, LAYERS, width), jnp.float32),
                vm((n_x, LAYERS * n_x, 128), jnp.float32),
                vm((LAYERS, 2, 2, rank, full), bf),
                vm((LAYERS, 2, rank, full), bf),
                vm((2, tokens, 2 * rank), jnp.float32),
                vm((tokens, width), jnp.float32),
                vm((tokens, 2 * rank), bf),
                vm((n_mp, n_x, rows, width), bf),
                vm((LAYERS, n_mp, 2, rows // 2, width), bf),
                vm((LAYERS, n_mp, 2, rows, width), bf),
                vm((LAYERS, n_mp, rows, width), bf),
                vm((n_mp, rows, width), bf),
                vm((LAYERS, len(BACK.single), rows, width), bf),
                vm((LAYERS, len(BACK.whole), n_x, rows, width), bf),
                dma((LAYERS, n_mp)),
                dma((LAYERS, n_mp, 3)),
                dma((n_mp,)),
                dma((3,)),
                dma((LAYERS, n_mp, 2)),
                dma((LAYERS, n_mp, 2)),
                dma((LAYERS, len(BACK.single))),
                dma((LAYERS, len(BACK.whole))),
                dma((LAYERS, 3)),
                dma((LAYERS, 3)),
                dma((LAYERS, 3)),
                dma((8,)),
            ],
            compiler_params=pltpu.CompilerParams(
                collective_id=0, has_side_effects=True, vmem_limit_bytes=60 * 1024 * 1024
            ),
        )(
            hidden_in,
            norm_gain,
            jnp.transpose(expert_ids, (0, 2, 1)),
            jnp.transpose(gate_counts, (0, 2, 1)),
            exit_layer[None, :],
            w_gate,
            w_up,
            w_down,
        )

    in_specs = (
        P(("groups", "expert", "dp"), "mp"),
        P(None, "mp"),
        P(None, ("groups", "expert", "dp"), None),
        P(None, ("groups", "expert", "dp"), None),
        P(("groups", "expert", "dp")),
        P(None, "expert", ("mp", "dp"), None),
        P(None, "expert", ("mp", "dp"), None),
        P(None, "expert", ("mp", "dp"), None),
    )
    out_specs = P(("groups", "expert", "dp"), "mp")
    return jax.shard_map(body, mesh=mesh, in_specs=in_specs, out_specs=out_specs, check_vma=False)
```

```python
import jax
import jax.numpy as jnp
from jax import lax
from jax.experimental import pallas as pl
from jax.experimental.pallas import tpu as pltpu
from jax.sharding import PartitionSpec as P

LAYERS = 2
NORM_FLOOR = 0.1
MESH = pl.DeviceIdType.MESH

OUT = {4: (0, False), 6: (4, False), 2: (0, False), 8: (6, False), 1: (0, True), 3: (4, True), 5: (4, True), 7: (6, False)}
BACK = {4: (0, False), 8: (4, False), 3: (0, False), 7: (4, False), 6: (4, False), 1: (0, False), 2: (1, True), 5: (4, True)}
OUT_DIRECT = (4, 6, 7, 8)
BACK_DIRECT = (1, 3, 4, 6, 7, 8)
OUT_PLAN = (
    ("z", 0), ("x", 0), ("z", 4), ("z", -4), ("z", 2), ("z", -2), ("z", 6), ("z", -6), ("m", 0), ("m", 4), ("x", 2), ("x", -2),
    ("m", -4), ("z", -7), ("z", 8), ("z", 7), ("m", 1), ("m", -1), ("m", -2), ("m", 2), ("m", -6), ("m", 3), ("m", 6), ("m", 5),
    ("m", -7), ("m", 8), ("m", -5), ("m", -3), ("m", 7),
)
BACK_PLAN = (
    ("m", 8), ("m", 5), ("m", -5), ("m", -7), ("m", 7), ("m", -6), ("m", 6), ("m", 2), ("m", -2), ("m", -3), ("m", 3), ("m", 0),
    ("z", 8), ("z", -7), ("z", 7), ("m", -4), ("m", 4), ("z", -6), ("z", 6), ("x", 0), ("m", -1), ("m", 1), ("z", -3), ("z", 3),
    ("z", -4), ("z", 4), ("z", 1), ("z", -1), ("z", 0),
)


class Tree:
    def __init__(self, half):
        self.parent, self.whole = {}, []
        for delta, (parent, whole) in half.items():
            for sign in (1,) if delta == 8 else (1, -1):
                self.parent[sign * delta] = sign * parent
                if whole:
                    self.whole.append(sign * delta)
        self.single = [delta for delta in self.parent if delta not in self.whole]
        self.order = [0, *self.parent]

    def below(self, delta, whole):
        among = self.whole if whole else self.single
        return [c for c in among if self.parent[c] == delta]

    def steps(self):
        return {s * (c - p) for c, p in self.parent.items() for s in (1, -1)}


OUT, BACK = Tree(OUT), Tree(BACK)
STEPS = sorted(OUT.steps() | BACK.steps())


def kernel(
    cur_in, gain_in, ids_in, counts_in, exit_in, wg_hbm, wu_hbm, wd_hbm, out_ref,
    acts, gains, routes, wgu, wdn, acc, ssq, hid, part, xa, xb, xc, stage, zin, zrow,
    zr, xr, gr, rr, xas, xbs, zs, zrs, lw, rw, sw, sends,
):
    m, e, d = lax.axis_index("mp"), lax.axis_index("expert"), lax.axis_index("dp")
    n_mp, n_x = acts.shape[1], acts.shape[2]
    rows, width = cur_in.shape
    half = rows // 2
    tokens = n_x * rows
    hidden = 2 * wdn.shape[2]
    full = n_mp * width

    def z(step):
        return {"mp": lax.rem(m + (step + n_mp), n_mp)}

    def x(step):
        return {"expert": lax.rem(e + (step + n_x), n_x)}

    partner = {"dp": 1 - d}
    em, ep, eo = (lax.rem(e + s, n_x) for s in (n_x - 1, 1, 2))

    def owner(delta):
        return lax.rem(m + (n_mp - delta), n_mp)

    def send(src, dst, ssem, rsem, dev):
        pltpu.make_async_remote_copy(
            src_ref=src, dst_ref=dst, send_sem=ssem, recv_sem=rsem, device_id=dev, device_id_type=MESH
        ).start()

    def await_bytes(ref, sem):
        pltpu.make_async_copy(ref, ref, sem).wait()

    def weight_parts(layer):
        return (
            (wg_hbm.at[layer, 0], lambda s: wgu.at[layer, 0, s], 0),
            (wu_hbm.at[layer, 0], lambda s: wgu.at[layer, 1, s], 1),
            (wd_hbm.at[layer, 0], lambda s: wdn.at[layer, s], 2),
        )

    def load_weights(layer):
        for src, dst, j in weight_parts(layer):
            pltpu.make_async_copy(src, dst(0), lw.at[layer, j]).start()

    def give_weights(layer):
        for src, dst, j in weight_parts(layer):
            send(src, dst(1), sw.at[layer, j], rw.at[layer, j], partner)

    barrier = pltpu.get_barrier_semaphore()
    peers = [z(h) for h in STEPS] + [x(1), x(-1), x(2), partner]
    for dev in peers:
        pl.semaphore_signal(barrier, inc=1, device_id=dev, device_id_type=MESH)
    load_weights(0)

    lines = []
    for layer in range(LAYERS):
        counts = counts_in[layer].astype(jnp.float32)
        share = counts / jnp.sum(counts, axis=0, keepdims=True)
        active = exit_in[...] > layer
        for expert in range(n_x):
            named = jnp.where((ids_in[layer] == expert) & active, share, 0.0)
            lines.append(jnp.sum(named, axis=0, keepdims=True))
    routes[e, :, 0:rows] = jnp.concatenate(lines, axis=0)
    routes[e, :, rows:] = jnp.zeros((LAYERS * n_x, routes.shape[2] - rows), jnp.float32)
    gains[m] = gain_in[...].astype(jnp.float32)
    acts[0, m, e] = cur_in[...]

    pl.semaphore_wait(barrier, len(peers))

    def layer_step(layer, carry):
        def spread(delta):
            i = OUT.order.index(delta)
            block = acts.at[layer, owner(delta), e]
            for child in OUT.below(delta, False):
                send(block, block, sends.at[0], zr.at[layer, OUT.order.index(child)], z(child - delta))
            send(block, block, sends.at[1], xr.at[layer, i, 0], x(1))
            send(block, block, sends.at[1], xr.at[layer, i, 1], x(-1))
            if abs(delta) in OUT_DIRECT:
                send(block, block, sends.at[1], xr.at[layer, i, 2], x(2))

            @pl.when(layer == 0)
            def _():
                gain = gains.at[owner(delta)]
                if delta != 0:
                    await_bytes(gain, gr.at[i])
                for child in OUT.below(delta, False) + OUT.below(delta, True):
                    send(gain, gain, sends.at[2], gr.at[OUT.order.index(child)], z(child - delta))

        def take_z(delta):
            if delta != 0:
                await_bytes(acts.at[layer, owner(delta), e], zr.at[layer, OUT.order.index(delta)])
            spread(delta)
            if delta == 0:

                @pl.when(layer == 0)
                def _():
                    for j, s in enumerate((1, -1, 2)):
                        send(routes.at[e], routes.at[e], sends.at[3], rr.at[j], x(s))
                    give_weights(0)

        def take_x(delta):
            i, k = OUT.order.index(delta), owner(delta)
            lo, hi = acts.at[layer, k, em], acts.at[layer, k, ep]
            await_bytes(lo, xr.at[layer, i, 0])
            piece = acts.at[layer, k, em, pl.ds(0, half)]
            send(piece, piece, sends.at[1], xr.at[layer, i, 2], x(1))
            await_bytes(hi, xr.at[layer, i, 1])
            piece = acts.at[layer, k, ep, pl.ds(half, half)]
            send(piece, piece, sends.at[1], xr.at[layer, i, 2], x(-1))

        def multiply(delta, first):
            i, k = OUT.order.index(delta), owner(delta)
            row = acts.at[layer, k]
            if delta in OUT.whole:
                await_bytes(row, zr.at[layer, i])

                @pl.when(layer == 0)
                def _():
                    await_bytes(gains.at[k], gr.at[i])

            else:
                if abs(delta) in OUT_DIRECT:
                    await_bytes(acts.at[layer, k, em], xr.at[layer, i, 0])
                    await_bytes(acts.at[layer, k, ep], xr.at[layer, i, 1])
                await_bytes(acts.at[layer, k, eo], xr.at[layer, i, 2])
            for child in OUT.below(delta, True):
                send(row, row, sends.at[6], zr.at[layer, OUT.order.index(child)], z(child - delta))
            block = acts[layer, k].reshape(tokens, width).astype(jnp.float32)
            squares = block * block
            scaled = (block * gains[k, pl.ds(layer, 1), :]).astype(jnp.bfloat16)
            at = pl.ds(pl.multiple_of(k * width, width), width)
            ssq[...] = squares if first else ssq[...] + squares

            def product(j):
                w = wgu[layer, j, :, :, at].reshape(hidden, width)
                p = lax.dot_general(scaled, w, (((1,), (1,)), ((), ())), preferred_element_type=jnp.float32)
                acc[j] = p if first else acc[j] + p

            for j in range(2):
                product(j)

        def weights_here(j):
            await_bytes(wdn.at[layer, 0], lw.at[layer, j])
            await_bytes(wdn.at[layer, 1], rw.at[layer, j])

        first = True
        for kind, delta in OUT_PLAN:
            if kind == "z":
                take_z(delta)
            elif kind == "x":
                take_x(delta)
            else:
                if first:
                    weights_here(0)
                    weights_here(1)
                multiply(delta, first)
                first = False

        @pl.when(layer == 0)
        def _():
            for j, s in enumerate((em, ep, eo)):
                await_bytes(routes.at[s], rr.at[j])
            load_weights(1)
            give_weights(1)

        eye = lax.broadcasted_iota(jnp.int32, (rows, rows), 0) == lax.broadcasted_iota(jnp.int32, (rows, rows), 1)
        columns = []
        for s in range(n_x):
            line = routes[s, pl.ds(layer * n_x + e, 1), 0:rows]
            columns.append(jnp.sum(jnp.where(eye, line, 0.0), axis=1, keepdims=True))
        weight = jnp.concatenate(columns, axis=0)
        inv = lax.rsqrt(jnp.sum(ssq[...], axis=1, keepdims=True) / full + NORM_FLOOR)
        gate = acc[0] * inv
        hid[...] = (gate / (1.0 + jnp.exp(-gate)) * (acc[1] * inv) * weight).astype(jnp.bfloat16)
        weights_here(2)

        def down(delta):
            i, f = BACK.order.index(delta), owner(delta)
            at = pl.ds(pl.multiple_of(f * width, width), width)
            w = wdn[layer, :, :, at].reshape(hidden, width)
            p = jnp.dot(hid[...], w, preferred_element_type=jnp.float32)
            for child in BACK.below(delta, True):
                j = BACK.whole.index(child)
                await_bytes(zrow.at[layer, j], zrs.at[layer, j])
                p = p + zrow[layer, j].reshape(tokens, width).astype(jnp.float32)
            part[f] = p.astype(jnp.bfloat16).reshape(n_x, rows, width)
            if delta in BACK.whole:
                j = BACK.whole.index(delta)
                send(part.at[f], zrow.at[layer, j], sends.at[7], zrs.at[layer, j], z(BACK.parent[delta] - delta))
                return
            if abs(delta) in BACK_DIRECT:
                send(part.at[f, eo], xc.at[layer, i], sends.at[4], xas.at[layer, i, 0], x(2))
                send(part.at[f, ep], xb.at[layer, i, 0], sends.at[4], xbs.at[layer, i, 0], x(1))
                send(part.at[f, em], xb.at[layer, i, 1], sends.at[4], xbs.at[layer, i, 1], x(-1))
                return
            send(part.at[f, eo, pl.ds(half, half)], xa.at[layer, i, 0], sends.at[4], xas.at[layer, i, 0], x(1))
            send(part.at[f, eo, pl.ds(0, half)], xa.at[layer, i, 1], sends.at[4], xas.at[layer, i, 1], x(-1))

        def merge_x(delta):
            i, f = BACK.order.index(delta), owner(delta)
            for side, (to, at, step) in enumerate(((ep, half, 1), (em, 0, -1))):
                await_bytes(xa.at[layer, i, side], xas.at[layer, i, side])
                old = part[f, to, at : at + half, :].astype(jnp.float32)
                new = old + xa[layer, i, side].astype(jnp.float32)
                part[f, to, at : at + half, :] = new.astype(jnp.bfloat16)
                send(part.at[f, to], xb.at[layer, i, side], sends.at[4], xbs.at[layer, i, side], x(step))

        def merge_z(delta):
            i, f = BACK.order.index(delta), owner(delta)
            for side in range(2):
                await_bytes(xb.at[layer, i, side], xbs.at[layer, i, side])
            total = part[f, e].astype(jnp.float32)
            for side in range(2):
                total = total + xb[layer, i, side].astype(jnp.float32)
            if abs(delta) in BACK_DIRECT:
                await_bytes(xc.at[layer, i], xas.at[layer, i, 0])
                total = total + xc[layer, i].astype(jnp.float32)
            for child in BACK.below(delta, False):
                j = BACK.single.index(child)
                await_bytes(zin.at[layer, j], zs.at[layer, j])
                total = total + zin[layer, j].astype(jnp.float32)
            if delta != 0:
                j = BACK.single.index(delta)
                stage[i] = total.astype(jnp.bfloat16)
                send(stage.at[i], zin.at[layer, j], sends.at[5], zs.at[layer, j], z(BACK.parent[delta] - delta))
                return
            new = (acts[layer, m, e].astype(jnp.float32) + total).astype(jnp.bfloat16)
            out_ref[...] = new

            @pl.when(layer == 0)
            def _():
                acts[1, m, e] = new

        for kind, delta in BACK_PLAN:
            if kind == "m":
                down(delta)
            elif kind == "x":
                merge_x(delta)
            else:
                merge_z(delta)

        for tree, at in ((OUT, (0, 1, 6)), (BACK, (5, 4, 7))):
            await_bytes(acts.at[layer, pl.ds(0, len(tree.single)), pl.ds(0, 1)], sends.at[at[0]])
            await_bytes(acts.at[layer, pl.ds(0, len(tree.single) + 1), pl.ds(0, 3)], sends.at[at[1]])
            await_bytes(acts.at[layer, pl.ds(0, len(tree.whole))], sends.at[at[2]])
        return carry

    lax.fori_loop(0, LAYERS, layer_step, 0)
    await_bytes(gains.at[pl.ds(0, n_mp - 1)], sends.at[2])
    await_bytes(routes.at[pl.ds(0, n_x - 1)], sends.at[3])
    for layer in range(LAYERS):
        for j in range(3):
            await_bytes(wdn.at[layer, 1], sw.at[layer, j])


def solution(mesh):
    n_mp, n_x = mesh.shape["mp"], mesh.shape["expert"]

    def body(hidden_in, norm_gain, expert_ids, gate_counts, exit_layer, w_gate, w_up, w_down):
        rows, width = hidden_in.shape
        _, _, rank, full = w_gate.shape
        tokens, bf = n_x * rows, jnp.bfloat16
        vm, dma = pltpu.VMEM, pltpu.SemaphoreType.DMA
        vmem = pl.BlockSpec(memory_space=pltpu.VMEM)
        hbm = pl.BlockSpec(memory_space=pl.ANY)
        return pl.pallas_call(
            kernel,
            out_shape=jax.ShapeDtypeStruct((rows, width), bf),
            in_specs=[vmem] * 5 + [hbm] * 3,
            out_specs=vmem,
            scratch_shapes=[
                vm((LAYERS, n_mp, n_x, rows, width), bf),
                vm((n_mp, LAYERS, width), jnp.float32),
                vm((n_x, LAYERS * n_x, 128), jnp.float32),
                vm((LAYERS, 2, 2, rank, full), bf),
                vm((LAYERS, 2, rank, full), bf),
                vm((2, tokens, 2 * rank), jnp.float32),
                vm((tokens, width), jnp.float32),
                vm((tokens, 2 * rank), bf),
                vm((n_mp, n_x, rows, width), bf),
                vm((LAYERS, n_mp, 2, rows // 2, width), bf),
                vm((LAYERS, n_mp, 2, rows, width), bf),
                vm((LAYERS, n_mp, rows, width), bf),
                vm((n_mp, rows, width), bf),
                vm((LAYERS, len(BACK.single), rows, width), bf),
                vm((LAYERS, len(BACK.whole), n_x, rows, width), bf),
                dma((LAYERS, n_mp)),
                dma((LAYERS, n_mp, 3)),
                dma((n_mp,)),
                dma((3,)),
                dma((LAYERS, n_mp, 2)),
                dma((LAYERS, n_mp, 2)),
                dma((LAYERS, len(BACK.single))),
                dma((LAYERS, len(BACK.whole))),
                dma((LAYERS, 3)),
                dma((LAYERS, 3)),
                dma((LAYERS, 3)),
                dma((8,)),
            ],
            compiler_params=pltpu.CompilerParams(
                collective_id=0, has_side_effects=True, vmem_limit_bytes=60 * 1024 * 1024
            ),
        )(
            hidden_in,
            norm_gain,
            jnp.transpose(expert_ids, (0, 2, 1)),
            jnp.transpose(gate_counts, (0, 2, 1)),
            exit_layer[None, :],
            w_gate,
            w_up,
            w_down,
        )

    in_specs = (
        P(("groups", "expert", "dp"), "mp"),
        P(None, "mp"),
        P(None, ("groups", "expert", "dp"), None),
        P(None, ("groups", "expert", "dp"), None),
        P(("groups", "expert", "dp")),
        P(None, "expert", ("mp", "dp"), None),
        P(None, "expert", ("mp", "dp"), None),
        P(None, "expert", ("mp", "dp"), None),
    )
    out_specs = P(("groups", "expert", "dp"), "mp")
    return jax.shard_map(body, mesh=mesh, in_specs=in_specs, out_specs=out_specs, check_vma=False)
```
